32 devices in a mesh: batch: 2 (over x), stage: 4 (over z), seq: 4 (over y, core).
Axes of the slice: x: 2, y: 2, z: 4, core: 2. Of those that a mesh axis runs over, the one named last changes fastest.
Arguments:
- tokens: bfloat16 [2, 4096, 2048], P('batch', 'seq'), parts along dimension 0
- w_q: bfloat16 [4, 2048, 2048], P('stage')
- w_k: bfloat16 [4, 2048, 2048], P('stage')
- w_v: bfloat16 [4, 2048, 4096], P('stage')
- w_a: bfloat16 [4, 2048, 8], P('stage')
- gate_bias: float32 [4, 8], P('stage')
- w_o: bfloat16 [4, 4096, 2048], P('stage')
- w_up: bfloat16 [4, 2048, 4096], P('stage')
- w_down: bfloat16 [4, 4096, 2048], P('stage')
- gain_attn: bfloat16 [4, 2048], P('stage')
- gain_mlp: bfloat16 [4, 2048], P('stage')
- gain_out: bfloat16 [4, 512], P('stage')
Outputs:
- output 1: bfloat16 [4, 2, 4096, 2048], P('stage', 'batch', 'seq'), parts along dimension 1
- output 2: float32 [4, 2, 8, 256, 512], P('stage', 'batch'), parts along dimension 1
There are 2 independent parts. The reference program is written for one: setup_inputs(seed, part) draws one part's arguments, and reference() takes and returns one part's arrays. A program takes and returns all parts, laid end to end along the dimension named above; an argument that names none is the same for every part.
All inputs are finite; a program needn't handle non-finite values.
Results may differ from the reference program's by a relative error of at most 0.02.
Values are sent between devices in bfloat16 or wider.
A program may use at most 1 GiB of HBM per device.

```python
import math
import functools
import jax
import jax.numpy as jnp
from jax import lax

BATCH_PART = 1
CHUNK_TOK = 1024
N_SHARDS = 4
N_LAYERS = 4
D_MODEL = 2048
N_HEADS = 8
K_HEAD = 256
V_HEAD = 512
FF_DIM = 4096

SEQ_LEN = N_SHARDS * CHUNK_TOK
QK_WIDTH = N_HEADS * K_HEAD
V_WIDTH = N_HEADS * V_HEAD
NORM_EPS = 1e-6


def draw_weight(rng_key, fan_in, arr_shape, mult_scale=1.0):
    raw_draw = jax.random.normal(rng_key, arr_shape, jnp.float32)
    return (mult_scale * fan_in ** -0.5 * raw_draw).astype(jnp.bfloat16)


def draw_gain(rng_key, arr_shape):
    return (1.0 + 0.3 * jax.random.normal(rng_key, arr_shape, jnp.float32)).astype(jnp.bfloat16)


def setup_inputs(seed: int = 0, part: int = 0) -> dict:
    base_key = jax.random.key(seed)
    key_list = jax.random.split(base_key, 11)
    noise_key, mean_key = jax.random.split(jax.random.fold_in(base_key, part), 2)
    tok_noise = jax.random.normal(noise_key, (BATCH_PART, SEQ_LEN, D_MODEL), jnp.float32)
    seq_mean = 0.7 * jax.random.normal(mean_key, (BATCH_PART, 1, D_MODEL), jnp.float32)
    bias_draw = jax.random.uniform(key_list[4], (N_LAYERS, N_HEADS), jnp.float32, 0.0, 1.5)
    return {
        "tokens": (tok_noise + seq_mean).astype(jnp.bfloat16),
        "w_q": draw_weight(key_list[0], D_MODEL, (N_LAYERS, D_MODEL, QK_WIDTH)),
        "w_k": draw_weight(key_list[1], D_MODEL, (N_LAYERS, D_MODEL, QK_WIDTH)),
        "w_v": draw_weight(key_list[2], D_MODEL, (N_LAYERS, D_MODEL, V_WIDTH)),
        "w_a": draw_weight(key_list[3], D_MODEL, (N_LAYERS, D_MODEL, N_HEADS), 0.7),
        "gate_bias": math.log(CHUNK_TOK) + bias_draw,
        "w_o": draw_weight(key_list[5], V_WIDTH, (N_LAYERS, V_WIDTH, D_MODEL)),
        "w_up": draw_weight(key_list[6], D_MODEL, (N_LAYERS, D_MODEL, FF_DIM)),
        "w_down": draw_weight(key_list[7], FF_DIM, (N_LAYERS, FF_DIM, D_MODEL)),
        "gain_attn": draw_gain(key_list[8], (N_LAYERS, D_MODEL)),
        "gain_mlp": draw_gain(key_list[9], (N_LAYERS, D_MODEL)),
        "gain_out": draw_gain(key_list[10], (N_LAYERS, V_HEAD)),
    }


def rms_scale(arr_in, gain_vec):
    arr_f32 = arr_in.astype(jnp.float32)
    inv_rms = lax.rsqrt(jnp.mean(arr_f32 * arr_f32, axis=-1, keepdims=True) + NORM_EPS)
    return arr_f32 * inv_rms * gain_vec.astype(jnp.float32)


def block_layer(layer_params, state_in, h_block):
    w_q, w_k, w_v, w_a, gate_bias, w_o, w_up, w_down, gain_attn, gain_mlp, gain_out = layer_params
    n_rows = BATCH_PART * CHUNK_TOK
    head_shape = (BATCH_PART, CHUNK_TOK, N_HEADS)
    u_flat = rms_scale(h_block, gain_attn).astype(jnp.bfloat16).reshape(n_rows, D_MODEL)
    query_h = jnp.dot(u_flat, w_q, preferred_element_type=jnp.float32).astype(jnp.bfloat16).reshape(head_shape + (K_HEAD,))
    key_s = (jnp.dot(u_flat, w_k, preferred_element_type=jnp.float32) * K_HEAD ** -0.5).astype(jnp.bfloat16).reshape(head_shape + (K_HEAD,))
    value_h = jnp.dot(u_flat, w_v, preferred_element_type=jnp.float32).astype(jnp.bfloat16).reshape(head_shape + (V_HEAD,))
    gate_logit = jnp.dot(u_flat, w_a, preferred_element_type=jnp.float32).reshape(head_shape) + gate_bias
    cum_decay = jnp.cumsum(jax.nn.log_sigmoid(gate_logit), axis=1)
    blk_decay = cum_decay[:, -1, :]
    scores = jnp.einsum("bthk,bjhk->bhtj", query_h.astype(jnp.float32), key_s.astype(jnp.float32))
    cum_heads = jnp.transpose(cum_decay, (0, 2, 1))
    decay_gap = cum_heads[:, :, :, None] - cum_heads[:, :, None, :]
    causal = jnp.arange(CHUNK_TOK)[:, None] >= jnp.arange(CHUNK_TOK)[None, :]
    mask_w = jnp.where(causal, jnp.exp(jnp.minimum(decay_gap, 0.0)), 0.0)
    attn_prob = (scores * mask_w).astype(jnp.bfloat16)
    o_intra = jnp.einsum("bhtj,bjhv->bthv", attn_prob.astype(jnp.float32), value_h.astype(jnp.float32))
    q_dec = (query_h.astype(jnp.float32) * jnp.exp(cum_decay)[..., None]).astype(jnp.bfloat16)
    state_bf = state_in.astype(jnp.bfloat16).astype(jnp.float32)
    o_inter = jnp.einsum("bthk,bhkv->bthv", q_dec.astype(jnp.float32), state_bf)
    k_dec = (key_s.astype(jnp.float32) * jnp.exp(blk_decay[:, None, :] - cum_decay)[..., None]).astype(jnp.bfloat16)
    local_state = jnp.einsum("bjhk,bjhv->bhkv", k_dec.astype(jnp.float32), value_h.astype(jnp.float32))
    state_out = jnp.exp(blk_decay)[:, :, None, None] * state_in + local_state
    o_norm = rms_scale(o_intra + o_inter, gain_out).astype(jnp.bfloat16).reshape(n_rows, V_WIDTH)
    attn_out = jnp.dot(o_norm, w_o, preferred_element_type=jnp.float32)
    u_mlp = rms_scale(h_block, gain_mlp).astype(jnp.bfloat16).reshape(n_rows, D_MODEL)
    hidden = jax.nn.gelu(jnp.dot(u_mlp, w_up, preferred_element_type=jnp.float32), approximate=True).astype(jnp.bfloat16)
    mlp_out = jnp.dot(hidden, w_down, preferred_element_type=jnp.float32)
    h_flat = h_block.astype(jnp.float32).reshape(n_rows, D_MODEL)
    h_new = (h_flat + attn_out + mlp_out).astype(jnp.bfloat16).reshape(BATCH_PART, CHUNK_TOK, D_MODEL)
    return state_out, h_new


def layer_apply(h_in, layer_params):
    h_blocks = jnp.transpose(h_in.reshape(BATCH_PART, N_SHARDS, CHUNK_TOK, D_MODEL), (1, 0, 2, 3))
    state_zero = jnp.zeros((BATCH_PART, N_HEADS, K_HEAD, V_HEAD), jnp.float32)
    state_fin, new_blocks = lax.scan(functools.partial(block_layer, layer_params), state_zero, h_blocks)
    h_new = jnp.transpose(new_blocks, (1, 0, 2, 3)).reshape(BATCH_PART, SEQ_LEN, D_MODEL)
    return h_new, (h_new, state_fin)


def reference(tokens, w_q, w_k, w_v, w_a, gate_bias, w_o, w_up, w_down, gain_attn, gain_mlp, gain_out):
    stacked = (w_q, w_k, w_v, w_a, gate_bias, w_o, w_up, w_down, gain_attn, gain_mlp, gain_out)
    _, (layer_out, final_state) = lax.scan(layer_apply, tokens, stacked)
    return layer_out, final_state
```

```python
import functools

import jax
import jax.numpy as jnp
from jax import lax
from jax.experimental import pallas as pl
from jax.experimental.pallas import tpu as pltpu
from jax.sharding import PartitionSpec as P

NORM_EPS = 1e-6
TILE = 256


def rms_scale(arr_in, gain_vec):
    arr_f32 = arr_in.astype(jnp.float32)
    inv_rms = lax.rsqrt(jnp.mean(arr_f32 * arr_f32, axis=-1, keepdims=True) + NORM_EPS)
    return arr_f32 * inv_rms * gain_vec.astype(jnp.float32)


def mm(lhs, rhs):
    return jnp.dot(lhs, rhs, preferred_element_type=jnp.float32)


def head_column(cum, head):
    lane = lax.broadcasted_iota(jnp.int32, cum.shape, 1)
    return jnp.sum(jnp.where(lane == head, cum, 0.0), axis=1, keepdims=True)


def gate_kernel(n_groups, *refs):
    logit_refs, bias_ref, cum_t_ref, cum_ref = refs[:n_groups], refs[n_groups], refs[n_groups + 1], refs[n_groups + 2]
    logit = jnp.concatenate([r[...] for r in logit_refs], axis=1) + bias_ref[...]
    run = jax.nn.log_sigmoid(logit)
    n_tok = run.shape[1]
    lane = lax.broadcasted_iota(jnp.int32, run.shape, 1)
    shift = 1
    while shift < n_tok:
        run = run + jnp.where(lane >= shift, pltpu.roll(run, shift, 1), 0.0)
        shift *= 2
    cum_t_ref[...] = run
    cum_ref[...] = run.T


def local_state_kernel(half_ref, k0_ref, k1_ref, v0_ref, v1_ref, cum_ref, out_ref):
    head = half_ref[0] * pl.num_programs(0) + pl.program_id(0)
    rows = k0_ref.shape[0]
    b_col = head_column(cum_ref[...], head)
    scale = jnp.exp(b_col[-1:, :] - b_col)
    total = None
    for idx, (k_ref, v_ref) in enumerate(((k0_ref, v0_ref), (k1_ref, v1_ref))):
        k_dec = (k_ref[...].astype(jnp.float32) * scale[idx * rows:(idx + 1) * rows, :]).astype(jnp.bfloat16)
        part = lax.dot_general(k_dec, v_ref[...], (((0,), (0,)), ((), ())), preferred_element_type=jnp.float32)
        total = part if total is None else total + part
    out_ref[0] = total


def attn_kernel(q0_ref, q1_ref, k0_ref, k1_ref, v0_ref, v1_ref, cum_ref, cum_t_ref, o0_ref, o1_ref):
    head = pl.program_id(0)
    rows = q0_ref.shape[0]
    per_group = rows // TILE
    b_col = head_column(cum_ref[...], head)
    b_row = cum_t_ref[pl.ds(head, 1), :]
    row_id = lax.broadcasted_iota(jnp.int32, (TILE, 1), 0)
    for tile in range(2 * per_group):
        grp, off = tile // per_group, (tile % per_group) * TILE
        q_tile = (q0_ref, q1_ref)[grp][off:off + TILE, :]
        b_tile = b_col[tile * TILE:(tile + 1) * TILE, :]
        total = None
        for src in range(grp + 1):
            n_col = rows if src < grp else off + TILE
            k_part = (k0_ref, k1_ref)[src][:n_col, :]
            v_part = (v0_ref, v1_ref)[src][:n_col, :]
            score = lax.dot_general(q_tile, k_part, (((1,), (1,)), ((), ())), preferred_element_type=jnp.float32)
            decay = jnp.exp(jnp.minimum(b_tile - b_row[:, src * rows:src * rows + n_col], 0.0))
            prob = score * decay
            if src == grp:
                col_id = lax.broadcasted_iota(jnp.int32, (1, n_col), 1)
                prob = jnp.where(row_id + off >= col_id, prob, 0.0)
            part = mm(prob.astype(jnp.bfloat16), v_part)
            total = part if total is None else total + part
        (o0_ref, o1_ref)[grp][off:off + TILE, :] = total


def out_norm_kernel(o_ref, q_ref, cum_ref, state_ref, gain_ref, out_ref):
    head = pl.program_id(0)
    b_col = head_column(cum_ref[...], head)
    q_dec = (q_ref[...].astype(jnp.float32) * jnp.exp(b_col)).astype(jnp.bfloat16)
    o_all = o_ref[...] + mm(q_dec, state_ref[0])
    inv_rms = lax.rsqrt(jnp.mean(o_all * o_all, axis=-1, keepdims=True) + NORM_EPS)
    out_ref[...] = (o_all * inv_rms * gain_ref[...].astype(jnp.float32)).astype(jnp.bfloat16)


def cost(flops, nbytes, trans=0):
    return pl.CostEstimate(flops=int(flops), bytes_accessed=int(nbytes), transcendentals=int(trans))


def run_gates(logits, gate_bias):
    n_heads, rows = logits[0].shape
    n_tok = rows * len(logits)
    return pl.pallas_call(
        functools.partial(gate_kernel, len(logits)),
        out_shape=(jax.ShapeDtypeStruct((n_heads, n_tok), jnp.float32), jax.ShapeDtypeStruct((n_tok, n_heads), jnp.float32)),
        cost_estimate=cost(40 * n_heads * n_tok, 700_000),
        name="gates",
    )(*logits, gate_bias[:, None])


def run_local_state(half, keys, values, cum):
    rows, k_all = keys[0].shape
    n_heads = cum.shape[1]
    k_head, v_head = k_all // n_heads, values[0].shape[1] // n_heads
    n_half = n_heads // 2

    def col_map(head, half_ref):
        return (0, half_ref[0] * n_half + head)

    k_spec = pl.BlockSpec((rows, k_head), col_map)
    v_spec = pl.BlockSpec((rows, v_head), col_map)
    return pl.pallas_call(
        local_state_kernel,
        grid_spec=pltpu.PrefetchScalarGridSpec(
            num_scalar_prefetch=1,
            grid=(n_half,),
            in_specs=[k_spec, k_spec, v_spec, v_spec, pl.BlockSpec(cum.shape, lambda head, half_ref: (0, 0))],
            out_specs=pl.BlockSpec((1, k_head, v_head), lambda head, half_ref: (head, 0, 0)),
        ),
        out_shape=jax.ShapeDtypeStruct((n_half, k_head, v_head), jnp.float32),
        cost_estimate=cost(4 * rows * k_head * v_head * n_half, 2 * 2 * rows * (k_head + v_head) * n_half + 4 * k_head * v_head * n_half),
        name="local_state",
    )(half, *keys, *values, cum)


def run_attn(queries, keys, values, cum, cum_t):
    rows, k_all = keys[0].shape
    n_heads = cum.shape[1]
    v_all = values[0].shape[1]
    k_head, v_head = k_all // n_heads, v_all // n_heads
    k_spec = pl.BlockSpec((rows, k_head), lambda head: (0, head))
    v_spec = pl.BlockSpec((rows, v_head), lambda head: (0, head))
    full = [pl.BlockSpec(cum.shape, lambda head: (0, 0)), pl.BlockSpec(cum_t.shape, lambda head: (0, 0))]
    o_shape = jax.ShapeDtypeStruct((rows, v_all), jnp.float32)
    n_pairs = 4 * rows * rows * 0.625
    return pl.pallas_call(
        attn_kernel,
        grid=(n_heads,),
        in_specs=[k_spec] * 4 + [v_spec] * 2 + full,
        out_specs=(v_spec, v_spec),
        out_shape=(o_shape, o_shape),
        cost_estimate=cost(2 * n_pairs * (k_all + v_all), 2 * 2 * rows * (2 * k_all + v_all) + 8 * rows * v_all, n_pairs * n_heads),
        name="block_attn",
    )(*queries, *keys, *values, cum, cum_t)


def run_out_norm(grp, o_part, query, cum, state_bf, gain_out):
    rows, v_all = o_part.shape
    n_heads = cum.shape[1]
    k_all = query.shape[1]
    k_head, v_head = k_all // n_heads, v_all // n_heads
    v_spec = pl.BlockSpec((rows, v_head), lambda head: (0, head))
    return pl.pallas_call(
        out_norm_kernel,
        grid=(n_heads,),
        in_specs=[
            v_spec,
            pl.BlockSpec((rows, k_head), lambda head: (0, head)),
            pl.BlockSpec((rows, n_heads), lambda head: (grp, 0)),
            pl.BlockSpec((1, k_head, v_head), lambda head: (head, 0, 0)),
            pl.BlockSpec((1, v_head), lambda head: (0, 0)),
        ],
        out_specs=v_spec,
        out_shape=jax.ShapeDtypeStruct((rows, v_all), jnp.bfloat16),
        cost_estimate=cost(2 * rows * k_head * v_all, rows * (6 * v_all + 2 * k_all) + 2 * k_all * v_head, rows * n_heads),
        name="out_norm",
    )(o_part, query, cum, state_bf, gain_out)


def solution(mesh):
    n_layers = mesh.shape["stage"]
    n_groups = 2
    stage_hop = [(src_idx, src_idx + 1) for src_idx in range(n_layers - 1)]
    core_swap = [(0, 1), (1, 0), (2, 3), (3, 2)]
    chip_swap = [(0, 2), (2, 0), (1, 3), (3, 1)]
    stacked = P("stage", None, None)
    per_layer = P("stage", None)

    def device_fn(tokens, w_q, w_k, w_v, w_a, gate_bias, w_o, w_up, w_down, gain_attn, gain_mlp, gain_out):
        stage_idx = lax.axis_index("stage")
        seq_idx = lax.axis_index("seq")
        core, chip = seq_idx % 2, seq_idx // 2
        is_even, is_first = core == 0, chip == 0
        w_q, w_k, w_v, w_a, w_o, w_up, w_down = (w[0] for w in (w_q, w_k, w_v, w_a, w_o, w_up, w_down))
        gate_bias, gain_attn, gain_mlp = gate_bias[0], gain_attn[0], gain_mlp[0]
        n_heads = w_a.shape[-1]
        k_head = w_q.shape[-1] // n_heads
        rows = tokens.shape[1] // n_groups
        half_own = core.astype(jnp.int32).reshape(1)
        half_other = 1 - half_own

        def mine(vec):
            n_half = n_heads // 2
            return jnp.where(is_even, vec[:n_half], vec[n_half:])[:, None, None]

        def project(h):
            u = rms_scale(h, gain_attn).astype(jnp.bfloat16)
            logit = lax.dot_general(w_a, u, (((0,), (1,)), ((), ())), preferred_element_type=jnp.float32)
            key = (mm(u, w_k) * k_head ** -0.5).astype(jnp.bfloat16)
            value = mm(u, w_v).astype(jnp.bfloat16)
            return u, logit, key, value

        def mlp_of(h):
            u_mlp = rms_scale(h, gain_mlp).astype(jnp.bfloat16)
            hidden = jax.nn.gelu(mm(u_mlp, w_up), approximate=True).astype(jnp.bfloat16)
            return mm(hidden, w_down)

        def query_of(u):
            return mm(u, w_q).astype(jnp.bfloat16)

        def layer(step, h_in, keep, fin):
            h0, h1 = h_in
            u0, logit0, key0, value0 = project(h0)
            query0 = query_of(u0)
            if step > 0:
                mlp0 = mlp_of(h0)
                h1, logit0, key0, value0, query0, mlp0 = lax.optimization_barrier((h1, logit0, key0, value0, query0, mlp0))
            u1, logit1, key1, value1 = project(h1)
            keys, values = (key0, key1), (value0, value1)
            cum_t, cum = run_gates((logit0, logit1), gate_bias)
            decay = cum_t[:, -1]
            loc_send = run_local_state(half_other, keys, values, cum)
            decay_peer = lax.ppermute(decay, "seq", core_swap)
            loc_peer = lax.ppermute(loc_send, "seq", core_swap)
            loc_own = run_local_state(half_own, keys, values, cum)
            query1 = query_of(u1)
            loc_peer, decay_peer, loc_own, query1 = lax.optimization_barrier((loc_peer, decay_peer, loc_own, query1))

            d_even, d_odd = jnp.where(is_even, decay, decay_peer), jnp.where(is_even, decay_peer, decay)
            l_even, l_odd = jnp.where(is_even, loc_own, loc_peer), jnp.where(is_even, loc_peer, loc_own)
            chip_state = jnp.exp(mine(d_odd)) * l_even + l_odd
            other_state = lax.ppermute(chip_state, "seq", chip_swap)
            d_chip = d_even + d_odd
            d_other = lax.ppermute(d_chip, "seq", chip_swap)

            queries = (query0, query1)
            o_intra = run_attn(queries, keys, values, cum, cum_t)
            if step == 0:
                mlp0 = mlp_of(h0)
            mlp1 = mlp_of(h1)
            o0, o1 = o_intra
            other_state, d_other, o0, o1, mlp0, mlp1 = lax.optimization_barrier((other_state, d_other, o0, o1, mlp0, mlp1))

            before = jnp.where(is_first, 0.0, other_state)
            s_odd = jnp.exp(mine(d_even)) * before + l_even
            s_own = jnp.where(is_even, before, s_odd).astype(jnp.bfloat16)
            s_give = jnp.where(is_even, s_odd, before).astype(jnp.bfloat16)
            s_peer = lax.ppermute(s_give, "seq", core_swap)
            state_bf = jnp.concatenate([jnp.where(is_even, s_own, s_peer), jnp.where(is_even, s_peer, s_own)], axis=0)

            def finish(g, h, o_part, mlp):
                o_norm = run_out_norm(g, o_part, queries[g], cum, state_bf, gain_out)
                h_new = (h.astype(jnp.float32) + mm(o_norm, w_o) + mlp).astype(jnp.bfloat16)
                return h_new, lax.ppermute(h_new, "stage", stage_hop) if step < n_layers - 1 else None

            is_mine = step == stage_idx
            new0, sent0 = finish(0, h0, o0, mlp0)
            new0, o1 = lax.optimization_barrier((new0, o1))
            new1, sent1 = finish(1, h1, o1, mlp1)
            keep_out = [new if keep is None else jnp.where(is_mine, new, keep[g]) for g, new in enumerate((new0, new1))]

            last_scale = jnp.exp(mine(jnp.where(is_first, d_other, d_chip)))
            first, last = jnp.where(is_first, chip_state, other_state), jnp.where(is_first, other_state, chip_state)
            fin_new = last_scale * first + last
            fin = fin_new if fin is None else jnp.where(is_mine, fin_new, fin)
            return (sent0, sent1), keep_out, fin

        h_cur = [tokens[0, g * rows:(g + 1) * rows] for g in range(n_groups)]
        keep = fin = None
        for step in range(n_layers):
            h_cur, keep, fin = layer(step, h_cur, keep, fin)
        fin_peer = lax.ppermute(fin, "seq", core_swap)
        fin_all = jnp.concatenate([jnp.where(is_even, fin, fin_peer), jnp.where(is_even, fin_peer, fin)], axis=0)
        return jnp.concatenate(keep, axis=0)[None, None], fin_all[None, None]

    in_specs = (P("batch", "seq", None), stacked, stacked, stacked, stacked, per_layer, stacked, stacked, stacked, per_layer, per_layer, per_layer)
    out_specs = (P("stage", "batch", "seq", None), P("stage", "batch", None, None, None))
    return jax.shard_map(device_fn, mesh=mesh, in_specs=in_specs, out_specs=out_specs, check_vma=False)
```
